32 devices in a mesh: dp: 8 (over z, core), ctx: 4 (over y, x).
Axes of the slice: x: 2, y: 2, z: 4, core: 2. Of those that a mesh axis runs over, the one named last changes fastest.
Arguments:
- state_rows: bfloat16 [12288, 2048], P(('dp', 'ctx')), parts along dimension 0, may hold values from -6 to 6
- query_vectors: bfloat16 [8, 12288, 128], P(None, ('dp', 'ctx')), parts along dimension 1, may hold values from -6 to 6
- key_vectors: bfloat16 [8, 12288, 128], P(None, ('dp', 'ctx')), parts along dimension 1, may hold values from -6 to 6
- value_vectors: bfloat16 [8, 12288, 128], P(None, ('dp', 'ctx')), parts along dimension 1, may hold values from -24 to 24
- halt_counts: int32 [12288], P(('dp', 'ctx')), parts along dimension 0, may hold values from 1 to 6, as said below
- out_weight: bfloat16 [8, 128, 2048], replicated, may hold values from -0.75 to 0.75
- norm_gain: bfloat16 [2048], replicated, may hold values from 0.099609375 to 1.8984375
Outputs:
- new_state: bfloat16 [12288, 2048], P(('dp', 'ctx')), parts along dimension 0
The draws below stay inside these ranges and needn't reach their ends.
There are 8 independent parts, one for each index of `dp`. The reference program is written for one: setup_inputs(seed, part) draws one part's arguments, and reference() takes and returns one part's arrays. A program takes and returns all parts, laid end to end along the dimension named above; an argument that names none is the same for every part. Nothing has to cross between parts.
Inputs may be any that keep to these rules, and one draw needn't show every extreme that they name: halt_counts is equal within each aligned tile of 128 positions; exactly 3 tiles of a document have counts above 2, and on some device of ctx all 3 tiles do.
All inputs are finite; a program needn't handle non-finite values.
Results may differ from the reference program's by a relative error of at most 0.008.
Values may be sent and summed in bfloat16 or wider, within the bound.
A program may use at most 128 MiB of HBM per device.

```python
import jax
import jax.numpy as jnp
from jax import lax

D = 2048
HEADS = 8
DH = 128
TILE = 128
STEP = 2
MAXSTEPS = 6
LEN = 1536
TILES_DEV = 3
ACTIVE = 3
HW = 1024
N_CTX = 4


def drawn_pair(key):
    key_query, key_key = jax.random.split(jax.random.fold_in(key, 7), 2)
    queries = jnp.clip(jax.random.normal(key_query, (HEADS, LEN, DH), jnp.float32), -6.0, 6.0)
    keys_all = jnp.clip(jax.random.normal(key_key, (HEADS, LEN, DH), jnp.float32), -6.0, 6.0)
    return (queries, keys_all)


def draw_query_vectors(key, part):
    return drawn_pair(key)[0].astype(jnp.bfloat16)


def draw_key_vectors(key, part):
    return drawn_pair(key)[1].astype(jnp.bfloat16)


def draw_halt_counts(key, part):
    key_priority, key_high, key_low, key_full = jax.random.split(jax.random.fold_in(key, 11), 4)
    tile_total = TILES_DEV * N_CTX
    full_device = jax.random.randint(key_full, (), 0, N_CTX)
    priority = jax.random.permutation(key_priority, tile_total).astype(jnp.int32)
    tile_device = jnp.arange(tile_total) // TILES_DEV
    priority = jnp.where(tile_device == full_device, -1, priority)
    ordering = jnp.argsort(priority, stable=True)
    active = jnp.zeros((tile_total,), jnp.int32).at[ordering[:ACTIVE]].set(1)
    high_counts = jax.random.randint(key_high, (tile_total,), STEP + 1, MAXSTEPS + 1)
    low_counts = jax.random.randint(key_low, (tile_total,), 1, STEP + 1)
    tile_counts = jnp.where(active == 1, high_counts, low_counts).astype(jnp.int32)
    return jnp.repeat(tile_counts, TILE, total_repeat_length=LEN)


def shard_levels(key, extent, shards, smallest, largest):
    gain = 1.0
    for position, parts in shards:
        heights = jax.random.uniform(jax.random.fold_in(jax.random.fold_in(key, 6), position), (parts,), jnp.float32, smallest / len(shards), largest / len(shards))
        gain = gain * jnp.repeat(jnp.exp(heights), extent[position] // parts).reshape((-1,) + (1,) * (len(extent) - 1 - position))
    return gain


def scatter_about(key, dims, deviation, bound, cuts=(), kind=jnp.bfloat16):
    result = jax.random.normal(key, dims, jnp.float32) * deviation
    if len(cuts) > 0:
        result = shard_levels(key, dims, cuts, -0.22, 0.18) * result
    return jnp.clip(result, min=-bound, max=bound).astype(kind)


def setup_inputs(seed: int = 0, part: int = 0) -> dict:
    key_list = jax.random.split(jax.random.key(seed), 8)
    own_keys = jax.random.split(jax.random.fold_in(key_list[7], part), 8)
    state_rows = scatter_about(own_keys[0], (LEN, D), 1.0, 6.0, ((0, 4),))
    query_vectors = draw_query_vectors(jax.random.fold_in(jax.random.fold_in(key_list[7], part), 71), part)
    key_vectors = draw_key_vectors(jax.random.fold_in(jax.random.fold_in(key_list[7], part), 71), part)
    value_vectors = scatter_about(own_keys[3], (HEADS, LEN, DH), 4.0, 24.0, ((1, 4),))
    halt_counts = draw_halt_counts(jax.random.fold_in(jax.random.fold_in(key_list[7], part), 71), part)
    out_weight = scatter_about(key_list[5], (HEADS, DH, D), (HW // 16) ** -0.5, 0.75)
    norm_gain = jnp.clip(1.0 + 0.18 * jax.random.normal(key_list[6], (D,), jnp.float32), 0.099609375, 1.8984375).astype(jnp.bfloat16)
    return {"state_rows": state_rows, "query_vectors": query_vectors, "key_vectors": key_vectors, "value_vectors": value_vectors, "halt_counts": halt_counts, "out_weight": out_weight, "norm_gain": norm_gain}


def reference(state_rows, query_vectors, key_vectors, value_vectors, halt_counts, out_weight, norm_gain):
    score_scale = DH ** (-0.5)

    def per_head(head_items):
        query_head, key_head, value_head = head_items
        scores = lax.dot_general(query_head, key_head, (((1,), (1,)), ((), ())), preferred_element_type=jnp.float32) * score_scale
        new_max = lax.optimization_barrier(jnp.max(scores, axis=1, keepdims=True))
        exponents = jnp.exp(scores - new_max)
        weight_sum = lax.optimization_barrier(jnp.sum(exponents, axis=1))
        weighted = jnp.dot(exponents.astype(jnp.bfloat16), value_head, preferred_element_type=jnp.float32)
        return (weighted / weight_sum[:, None]).astype(jnp.bfloat16)
    attended = lax.map(per_head, (query_vectors, key_vectors, value_vectors))
    update = jnp.einsum('hqd,hde->qe', attended.astype(jnp.float32), out_weight.astype(jnp.float32))
    mixed_sum = state_rows.astype(jnp.float32) + update
    normed = mixed_sum * lax.rsqrt(lax.optimization_barrier(jnp.mean(mixed_sum * mixed_sum, axis=-1, keepdims=True)) + 1e-06) * norm_gain.astype(jnp.float32)
    active = (halt_counts > STEP)[:, None]
    return jnp.where(active, normed.astype(jnp.bfloat16), state_rows)
```

```python
import functools

import jax
import jax.numpy as jnp
from jax import lax
from jax.experimental import pallas as pl
from jax.experimental.pallas import tpu as pltpu
from jax.sharding import PartitionSpec as P

STEP = 2
TILE = 128
LOG2E = 1.4426950408889634


def peer_of(me, step, n):
    peer = 0
    bit = 1
    while bit < n:
        digit = (me // bit) % 2
        if step & bit:
            digit = (digit + 1) % 2
        peer = peer + digit * bit
        bit *= 2
    return peer


def split_kernel(
    n,
    share,
    q_hbm,
    k_hbm,
    v_hbm,
    flag_hbm,
    state_hbm,
    w_hbm,
    gain_ref,
    out_ref,
    q_buf,
    k_buf,
    v_buf,
    flag_buf,
    state_buf,
    w_buf,
    probs,
    inv_sum,
    att_buf,
    update,
    send_sem,
    recv_sem,
    att_send,
    att_recv,
    local_sem,
    big_sem,
):
    me = lax.axis_index("ctx")
    rows, width = q_hbm.shape[1], q_hbm.shape[2]
    scale = width ** (-0.5) * LOG2E
    peers = [peer_of(me, step, n) for step in range(n)]

    def mine(ref, device):
        return ref.at[pl.ds(device * share, share)]

    tensors = ((k_hbm, k_buf), (q_hbm, q_buf), (v_hbm, v_buf))
    own = []
    for index, (src, buf) in enumerate(tensors):
        own.append(pltpu.make_async_copy(mine(src, me), buf.at[me], local_sem.at[index]))
    own.append(pltpu.make_async_copy(flag_hbm, flag_buf.at[me], local_sem.at[3]))
    for copy in own:
        copy.start()

    barrier = pltpu.get_barrier_semaphore()
    for step in range(1, n):
        pl.semaphore_signal(
            barrier, inc=1, device_id={"ctx": peers[step]}, device_id_type=pl.DeviceIdType.MESH
        )
    pl.semaphore_wait(barrier, n - 1)

    order = list(range(n - 1, 0, -1))

    def remote(src, dst, send, recv, step):
        return pltpu.make_async_remote_copy(
            src_ref=src,
            dst_ref=dst,
            send_sem=send,
            recv_sem=recv,
            device_id={"ctx": peers[step]},
            device_id_type=pl.DeviceIdType.MESH,
        )

    sends = {}
    for step in order:
        sends[3, step] = remote(
            flag_hbm, flag_buf.at[me], send_sem.at[3, step], recv_sem.at[3, step], step
        )
        sends[3, step].start()
    for index, (src, buf) in enumerate(tensors):
        for step in order:
            sends[index, step] = remote(
                mine(src, peers[step]),
                buf.at[me],
                send_sem.at[index, step],
                recv_sem.at[index, step],
                step,
            )
            sends[index, step].start()

    w_copy = pltpu.make_async_copy(w_hbm, w_buf, big_sem.at[0])
    w_copy.start()
    state_copy = pltpu.make_async_copy(state_hbm, state_buf, big_sem.at[1])
    state_copy.start()

    for index in (3, 0, 1):
        own[index].wait()
        for step in order:
            sends[index, step].wait_recv()

    for h in range(share):
        chosen = None
        for src in range(n):
            term = q_buf[src, h].astype(jnp.float32) * flag_buf[src, 0:1, :]
            chosen = term if chosen is None else chosen + term
        queries = chosen.astype(jnp.bfloat16)
        for block in range(rows // TILE):
            part = queries[block * TILE : (block + 1) * TILE]
            scores = [
                lax.dot_general(
                    part,
                    k_buf[src, h],
                    (((1,), (1,)), ((), ())),
                    preferred_element_type=jnp.float32,
                )
                for src in range(n)
            ]
            top = jnp.max(scores[0], axis=1, keepdims=True)
            for piece in scores[1:]:
                top = jnp.maximum(top, jnp.max(piece, axis=1, keepdims=True))
            total = None
            for src, piece in enumerate(scores):
                weights = jnp.exp2((piece - top) * scale)
                term = jnp.sum(weights, axis=1, keepdims=True)
                total = term if total is None else total + term
                probs[h, src, block * TILE : (block + 1) * TILE, :] = weights.astype(jnp.bfloat16)
            inv_sum[h, block * TILE : (block + 1) * TILE, :] = jnp.broadcast_to(
                1.0 / total, (TILE, width)
            )

    own[2].wait()
    for step in order:
        sends[2, step].wait_recv()

    for h in range(share):
        weighted = None
        for src in range(n):
            term = jnp.dot(probs[h, src], v_buf[src, h], preferred_element_type=jnp.float32)
            weighted = term if weighted is None else weighted + term
        att_buf[me, :, h * width : (h + 1) * width] = (weighted * inv_sum[h]).astype(jnp.bfloat16)

    att_sends = {}
    for step in order:
        att_sends[step] = remote(
            att_buf.at[me], att_buf.at[me], att_send.at[step], att_recv.at[step], step
        )
        att_sends[step].start()

    w_copy.wait()
    state_copy.wait()
    span = share * width

    def project(source, first):
        def body(block, carry):
            cut = pl.ds(pl.multiple_of(block * TILE, TILE), TILE)
            weight = w_buf[pl.ds(pl.multiple_of(source * span, span), span), :]
            product = jnp.dot(att_buf[source, cut, :], weight, preferred_element_type=jnp.float32)
            if first:
                update[cut, :] = state_buf[cut, :].astype(jnp.float32) + product
            else:
                update[cut, :] = update[cut, :] + product
            return carry

        lax.fori_loop(0, rows // TILE, body, 0)

    project(me, True)
    for step in range(1, n):
        att_sends[step].wait_recv()
        project(peers[step], False)

    gain = gain_ref[...].astype(jnp.float32)
    piece_rows = 32

    def finish(block, carry):
        cut = pl.ds(pl.multiple_of(block * piece_rows, piece_rows), piece_rows)
        mixed = update[cut, :]
        mean = jnp.mean(mixed * mixed, axis=-1, keepdims=True)
        out_ref[cut, :] = (mixed * lax.rsqrt(mean + 1e-06) * gain).astype(out_ref.dtype)
        return carry

    lax.fori_loop(0, rows // piece_rows, finish, 0)

    for copy in sends.values():
        copy.wait_send()
    for copy in att_sends.values():
        copy.wait_send()


def split_heads(n, state_rows, q, k, v, halt_counts, out_weight, norm_gain):
    heads, rows, width = q.shape
    share = heads // n
    features = state_rows.shape[1]
    flag = jnp.broadcast_to((halt_counts[0] > STEP).astype(jnp.float32), (8, 128))
    bf16, f32 = jnp.bfloat16, jnp.float32
    anywhere = pl.BlockSpec(memory_space=pl.ANY)
    vmem = pl.BlockSpec(memory_space=pltpu.VMEM)
    block = pltpu.VMEM((n, share, rows, width), bf16)
    normed = pl.pallas_call(
        functools.partial(split_kernel, n, share),
        out_shape=jax.ShapeDtypeStruct((rows, features), bf16),
        in_specs=[anywhere] * 6 + [vmem],
        out_specs=vmem,
        scratch_shapes=[
            block,
            block,
            block,
            pltpu.VMEM((n, 8, 128), f32),
            pltpu.VMEM((rows, features), bf16),
            pltpu.VMEM((heads * width, features), bf16),
            pltpu.VMEM((share, n, rows, rows), bf16),
            pltpu.VMEM((share, rows, width), f32),
            pltpu.VMEM((n, rows, share * width), bf16),
            pltpu.VMEM((rows, features), f32),
            pltpu.SemaphoreType.DMA((4, n)),
            pltpu.SemaphoreType.DMA((4, n)),
            pltpu.SemaphoreType.DMA((n,)),
            pltpu.SemaphoreType.DMA((n,)),
            pltpu.SemaphoreType.DMA((4,)),
            pltpu.SemaphoreType.DMA((2,)),
        ],
        compiler_params=pltpu.CompilerParams(
            collective_id=0, has_side_effects=True, vmem_limit_bytes=40 * 1024 * 1024
        ),
    )(
        q,
        k,
        v,
        flag,
        state_rows,
        out_weight.reshape(heads * width, features),
        norm_gain.reshape(1, features),
    )
    active = (halt_counts > STEP)[:, None]
    return jnp.where(active, normed, state_rows)


def fold_heads(carry, queries, key_piece, value_piece, score_scale):
    running_max, running_sum, weighted = carry

    def per_head(head_items):
        query_head, key_head, value_head, max_head, sum_head, weighted_head = head_items
        scores = (
            lax.dot_general(
                query_head, key_head, (((1,), (1,)), ((), ())), preferred_element_type=jnp.float32
            )
            * score_scale
        )
        new_max = jnp.maximum(max_head, jnp.max(scores, axis=1))
        shrink = jnp.exp(max_head - new_max)
        exponents = jnp.exp(scores - new_max[:, None])
        sum_head = sum_head * shrink + jnp.sum(exponents, axis=1)
        weighted_head = weighted_head * shrink[:, None] + jnp.dot(
            exponents.astype(jnp.bfloat16), value_head, preferred_element_type=jnp.float32
        )
        return (new_max, sum_head, weighted_head)

    return lax.map(per_head, (queries, key_piece, value_piece, running_max, running_sum, weighted))


def empty_carry(head_count, query_count, head_width):
    return (
        jnp.full((head_count, query_count), -1e30, jnp.float32),
        jnp.zeros((head_count, query_count), jnp.float32),
        jnp.zeros((head_count, query_count, head_width), jnp.float32),
    )


def attend_keys(query_vectors, key_vectors, value_vectors, score_scale):
    head_count, row_count, head_width = query_vectors.shape
    initial = empty_carry(head_count, row_count, head_width)
    running_max, running_sum, weighted = fold_heads(
        initial,
        query_vectors,
        lax.all_gather(key_vectors, "ctx", axis=1, tiled=True),
        lax.all_gather(value_vectors, "ctx", axis=1, tiled=True),
        score_scale,
    )
    return (weighted / running_sum[..., None]).astype(jnp.bfloat16)


def on_device(
    state_rows, query_vectors, key_vectors, value_vectors, halt_counts, out_weight, norm_gain
):
    head_count, row_count, head_width = query_vectors.shape
    score_scale = head_width ** (-0.5)
    attended = attend_keys(query_vectors, key_vectors, value_vectors, score_scale)
    update = jnp.einsum("hqd,hde->qe", attended, out_weight, preferred_element_type=jnp.float32)
    mixed_sum = state_rows.astype(jnp.float32) + update
    normed = (
        mixed_sum
        * lax.rsqrt(jnp.mean(mixed_sum * mixed_sum, axis=-1, keepdims=True) + 1e-06)
        * norm_gain.astype(jnp.float32)
    )
    active = (halt_counts > STEP)[:, None]
    return jnp.where(active, normed.astype(jnp.bfloat16), state_rows)


def solution(mesh):
    n_ctx = mesh.shape["ctx"]

    def per_device(state_rows, q, k, v, halt_counts, out_weight, norm_gain):
        heads, rows, _ = q.shape
        one_owner = rows == (n_ctx - 1) * TILE
        if one_owner and heads % n_ctx == 0 and n_ctx & (n_ctx - 1) == 0:
            return split_heads(n_ctx, state_rows, q, k, v, halt_counts, out_weight, norm_gain)
        return on_device(state_rows, q, k, v, halt_counts, out_weight, norm_gain)

    placed = (
        P(("dp", "ctx"), None),
        P(None, ("dp", "ctx"), None),
        P(None, ("dp", "ctx"), None),
        P(None, ("dp", "ctx"), None),
        P(("dp", "ctx")),
        P(),
        P(),
    )
    return jax.shard_map(
        per_device, mesh=mesh, in_specs=placed, out_specs=P(("dp", "ctx"), None), check_vma=False
    )
```

```python
import functools

import jax
import jax.numpy as jnp
from jax import lax
from jax.experimental import pallas as pl
from jax.experimental.pallas import tpu as pltpu
from jax.sharding import PartitionSpec as P

STEP = 2
TILE = 128
LOG2E = 1.4426950408889634


def peer_of(me, step, n):
    peer = 0
    bit = 1
    while bit < n:
        digit = (me // bit) % 2
        if step & bit:
            digit = (digit + 1) % 2
        peer = peer + digit * bit
        bit *= 2
    return peer


def split_kernel(
    n,
    share,
    halt_ref,
    q_hbm,
    k_hbm,
    v_hbm,
    state_hbm,
    w_hbm,
    gain_ref,
    out_ref,
    q_buf,
    k_buf,
    v_buf,
    flag_out,
    flag_buf,
    state_buf,
    w_buf,
    probs,
    inv_sum,
    att_buf,
    update,
    send_sem,
    recv_sem,
    flag_send,
    flag_recv,
    att_send,
    att_recv,
    local_sem,
    w_sem,
    state_sem,
):
    me = lax.axis_index("ctx")
    rows, width = q_hbm.shape[1], q_hbm.shape[2]
    blocks = rows // TILE
    scale = width ** (-0.5) * LOG2E
    peers = [peer_of(me, step, n) for step in range(n)]
    order = list(range(n - 1, 0, -1))
    tensors = ((k_hbm, k_buf), (q_hbm, q_buf), (v_hbm, v_buf))
    own_rows = pl.ds(pl.multiple_of(me * rows, rows), rows)
    own_lanes = pl.ds(pl.multiple_of(me * width, width), width)

    flag = jnp.full(flag_out.shape, halt_ref[0] > STEP).astype(jnp.float32)
    flag_out[...] = flag

    own = {}
    for h in range(share):
        for index, (src, buf) in enumerate(tensors):
            own[index, h] = pltpu.make_async_copy(
                src.at[me * share + h], buf.at[h, own_rows], local_sem.at[index, h]
            )
            own[index, h].start()

    barrier = pltpu.get_barrier_semaphore()
    for step in range(1, n):
        pl.semaphore_signal(
            barrier, inc=1, device_id={"ctx": peers[step]}, device_id_type=pl.DeviceIdType.MESH
        )
    pl.semaphore_wait(barrier, n - 1)

    def remote(src, dst, send, recv, step):
        copy = pltpu.make_async_remote_copy(
            src_ref=src,
            dst_ref=dst,
            send_sem=send,
            recv_sem=recv,
            device_id={"ctx": peers[step]},
            device_id_type=pl.DeviceIdType.MESH,
        )
        copy.start()
        return copy

    sends, flags, gathers = {}, {}, {}
    for h in range(share):
        for index, (src, buf) in enumerate(tensors):
            for step in order:
                sends[index, h, step] = remote(
                    src.at[peers[step] * share + h],
                    buf.at[h, own_rows],
                    send_sem.at[index, h, step],
                    recv_sem.at[index, h, step],
                    step,
                )
            if h == 0 and index == 0:
                for step in order:
                    flags[step] = remote(
                        flag_out, flag_buf.at[me], flag_send.at[step], flag_recv.at[step], step
                    )

    w_copies = []
    for head in range(n * share):
        w_copies.append(
            pltpu.make_async_copy(
                w_hbm.at[head],
                w_buf.at[head % share, pl.ds((head // share) * width, width)],
                w_sem.at[head],
            )
        )
        w_copies[-1].start()
    state_copy = pltpu.make_async_copy(state_hbm, state_buf, state_sem)
    state_copy.start()

    def arrived(index, h):
        own[index, h].wait()
        for step in order:
            sends[index, h, step].wait_recv()

    def gather(h, block):
        if block is None:
            cut, slot = pl.ds(0, rows), 0
        else:
            cut, slot = pl.ds(block * TILE, TILE), block
        for step in order:
            gathers[h, slot, step] = remote(
                att_buf.at[h, cut, own_lanes],
                att_buf.at[h, cut, own_lanes],
                att_send.at[h, slot, step],
                att_recv.at[h, slot, step],
                step,
            )

    for h in range(share):
        arrived(0, h)
        arrived(1, h)
        if h == 0:
            for step in order:
                flags[step].wait_recv()
        for block in range(blocks):
            base = block * TILE
            chosen = q_buf[h, pl.ds(pl.multiple_of(me * rows, rows) + base, TILE), :].astype(jnp.float32) * flag[0:1, :]
            for step in order:
                start = pl.multiple_of(peers[step] * rows, rows) + base
                term = q_buf[h, pl.ds(start, TILE), :].astype(jnp.float32)
                chosen = chosen + term * flag_buf[peers[step], 0:1, :]
            scores = lax.dot_general(
                chosen.astype(jnp.bfloat16),
                k_buf[h],
                (((1,), (1,)), ((), ())),
                preferred_element_type=jnp.float32,
            )
            top = jnp.max(scores, axis=1, keepdims=True)
            weights = jnp.exp2((scores - top) * scale)
            total = jnp.sum(weights, axis=1, keepdims=True)
            probs[base : base + TILE, :] = weights.astype(jnp.bfloat16)
            inv_sum[base : base + TILE, :] = jnp.broadcast_to(1.0 / total, (TILE, width))
        arrived(2, h)
        last = h == share - 1
        for block in range(blocks):
            cut = slice(block * TILE, (block + 1) * TILE)
            weighted = jnp.dot(probs[cut, :], v_buf[h], preferred_element_type=jnp.float32)
            att_buf[h, cut, own_lanes] = (weighted * inv_sum[cut, :]).astype(jnp.bfloat16)
            if last:
                gather(h, block)
        if not last:
            gather(h, None)

    for copy in w_copies:
        copy.wait()
    state_copy.wait()

    for h in range(share - 1):
        for step in order:
            gathers[h, 0, step].wait_recv()

        def body(block, carry, h=h):
            cut = pl.ds(pl.multiple_of(block * TILE, TILE), TILE)
            product = jnp.dot(att_buf[h, cut, :], w_buf[h], preferred_element_type=jnp.float32)
            if h == 0:
                update[cut, :] = state_buf[cut, :].astype(jnp.float32) + product
            else:
                update[cut, :] = update[cut, :] + product
            return carry

        lax.fori_loop(0, blocks, body, 0)

    gain = gain_ref[...].astype(jnp.float32).reshape(1, -1)
    h = share - 1
    for block in range(blocks):
        for step in order:
            gathers[h, block, step].wait_recv()
        cut = slice(block * TILE, (block + 1) * TILE)
        mixed = jnp.dot(att_buf[h, cut, :], w_buf[h], preferred_element_type=jnp.float32)
        residual = update if share > 1 else state_buf
        mixed = residual[cut, :].astype(jnp.float32) + mixed
        mean = jnp.mean(mixed * mixed, axis=-1, keepdims=True)
        out_ref[cut, :] = (mixed * lax.rsqrt(mean + 1e-06) * gain).astype(out_ref.dtype)

    for group in (sends, flags, gathers):
        for copy in group.values():
            copy.wait_send()


def split_heads(n, state_rows, q, k, v, halt_counts, out_weight, norm_gain):
    heads, rows, width = q.shape
    share = heads // n
    features = state_rows.shape[1]
    bf16, f32 = jnp.bfloat16, jnp.float32
    hbm = pl.BlockSpec(memory_space=pltpu.MemorySpace.HBM)
    vmem = pl.BlockSpec(memory_space=pltpu.VMEM)
    block = pltpu.VMEM((share, n * rows, width), bf16)
    dma = pltpu.SemaphoreType.DMA
    normed = pl.pallas_call(
        functools.partial(split_kernel, n, share),
        out_shape=jax.ShapeDtypeStruct((rows, features), bf16),
        in_specs=[pl.BlockSpec(memory_space=pltpu.SMEM)] + [hbm] * 5 + [vmem],
        out_specs=vmem,
        scratch_shapes=[
            block,
            block,
            block,
            pltpu.VMEM((8, 128), f32),
            pltpu.VMEM((n, 8, 128), f32),
            pltpu.VMEM((rows, features), bf16),
            pltpu.VMEM((share, n * width, features), bf16),
            pltpu.VMEM((rows, n * rows), bf16),
            pltpu.VMEM((rows, width), f32),
            pltpu.VMEM((share, rows, n * width), bf16),
            pltpu.VMEM((rows, features), f32),
            dma((3, share, n)),
            dma((3, share, n)),
            dma((n,)),
            dma((n,)),
            dma((share, rows // TILE, n)),
            dma((share, rows // TILE, n)),
            dma((3, share)),
            dma((heads,)),
            dma,
        ],
        compiler_params=pltpu.CompilerParams(
            collective_id=0, has_side_effects=True, vmem_limit_bytes=60 * 1024 * 1024
        ),
    )(halt_counts, q, k, v, state_rows, out_weight, norm_gain)
    active = (halt_counts > STEP)[:, None]
    return jnp.where(active, normed, state_rows)


def fold_heads(carry, queries, key_piece, value_piece, score_scale):
    running_max, running_sum, weighted = carry

    def per_head(head_items):
        query_head, key_head, value_head, max_head, sum_head, weighted_head = head_items
        scores = (
            lax.dot_general(
                query_head, key_head, (((1,), (1,)), ((), ())), preferred_element_type=jnp.float32
            )
            * score_scale
        )
        new_max = jnp.maximum(max_head, jnp.max(scores, axis=1))
        shrink = jnp.exp(max_head - new_max)
        exponents = jnp.exp(scores - new_max[:, None])
        sum_head = sum_head * shrink + jnp.sum(exponents, axis=1)
        weighted_head = weighted_head * shrink[:, None] + jnp.dot(
            exponents.astype(jnp.bfloat16), value_head, preferred_element_type=jnp.float32
        )
        return (new_max, sum_head, weighted_head)

    return lax.map(per_head, (queries, key_piece, value_piece, running_max, running_sum, weighted))


def empty_carry(head_count, query_count, head_width):
    return (
        jnp.full((head_count, query_count), -1e30, jnp.float32),
        jnp.zeros((head_count, query_count), jnp.float32),
        jnp.zeros((head_count, query_count, head_width), jnp.float32),
    )


def attend_keys(query_vectors, key_vectors, value_vectors, score_scale):
    head_count, row_count, head_width = query_vectors.shape
    initial = empty_carry(head_count, row_count, head_width)
    running_max, running_sum, weighted = fold_heads(
        initial,
        query_vectors,
        lax.all_gather(key_vectors, "ctx", axis=1, tiled=True),
        lax.all_gather(value_vectors, "ctx", axis=1, tiled=True),
        score_scale,
    )
    return (weighted / running_sum[..., None]).astype(jnp.bfloat16)


def on_device(
    state_rows, query_vectors, key_vectors, value_vectors, halt_counts, out_weight, norm_gain
):
    head_count, row_count, head_width = query_vectors.shape
    score_scale = head_width ** (-0.5)
    attended = attend_keys(query_vectors, key_vectors, value_vectors, score_scale)
    update = jnp.einsum("hqd,hde->qe", attended, out_weight, preferred_element_type=jnp.float32)
    mixed_sum = state_rows.astype(jnp.float32) + update
    normed = (
        mixed_sum
        * lax.rsqrt(jnp.mean(mixed_sum * mixed_sum, axis=-1, keepdims=True) + 1e-06)
        * norm_gain.astype(jnp.float32)
    )
    active = (halt_counts > STEP)[:, None]
    return jnp.where(active, normed.astype(jnp.bfloat16), state_rows)


def solution(mesh):
    n_ctx = mesh.shape["ctx"]

    def per_device(state_rows, q, k, v, halt_counts, out_weight, norm_gain):
        heads, rows, _ = q.shape
        one_owner = rows == (n_ctx - 1) * TILE
        if one_owner and heads % n_ctx == 0 and n_ctx & (n_ctx - 1) == 0:
            return split_heads(n_ctx, state_rows, q, k, v, halt_counts, out_weight, norm_gain)
        return on_device(state_rows, q, k, v, halt_counts, out_weight, norm_gain)

    placed = (
        P(("dp", "ctx"), None),
        P(None, ("dp", "ctx"), None),
        P(None, ("dp", "ctx"), None),
        P(None, ("dp", "ctx"), None),
        P(("dp", "ctx")),
        P(),
        P(),
    )
    return jax.shard_map(
        per_device, mesh=mesh, in_specs=placed, out_specs=P(("dp", "ctx"), None), check_vma=False
    )
```

```python
import functools

import jax
import jax.numpy as jnp
from jax import lax
from jax.experimental import pallas as pl
from jax.experimental.pallas import tpu as pltpu
from jax.sharding import PartitionSpec as P

STEP = 2
TILE = 128
LOG2E = 1.4426950408889634


def peer_of(me, step, n):
    peer = 0
    bit = 1
    while bit < n:
        digit = (me // bit) % 2
        if step & bit:
            digit = (digit + 1) % 2
        peer = peer + digit * bit
        bit *= 2
    return peer


def split_kernel(
    n,
    share,
    halt_ref,
    q_hbm,
    k_hbm,
    v_hbm,
    state_hbm,
    w_hbm,
    gain_ref,
    out_ref,
    q_buf,
    k_buf,
    v_buf,
    flag_out,
    flag_buf,
    state_buf,
    w_buf,
    probs,
    inv_sum,
    att_buf,
    update,
    send_sem,
    recv_sem,
    flag_send,
    flag_recv,
    att_send,
    att_recv,
    local_sem,
    w_sem,
    state_sem,
):
    me = lax.axis_index("ctx")
    rows, width = q_hbm.shape[1], q_hbm.shape[2]
    blocks = rows // TILE
    scale = width ** (-0.5) * LOG2E
    peers = [peer_of(me, step, n) for step in range(n)]
    order = list(range(n - 1, 0, -1))
    tensors = ((k_hbm, k_buf), (q_hbm, q_buf), (v_hbm, v_buf))
    own_rows = pl.ds(pl.multiple_of(me * rows, rows), rows)
    own_lanes = pl.ds(pl.multiple_of(me * width, width), width)

    flag = jnp.full(flag_out.shape, halt_ref[0] > STEP).astype(jnp.float32)
    flag_out[...] = flag

    own = {}
    for h in range(share):
        for index, (src, buf) in enumerate(tensors):
            own[index, h] = pltpu.make_async_copy(
                src.at[me * share + h], buf.at[h, own_rows], local_sem.at[index, h]
            )
            own[index, h].start()

    barrier = pltpu.get_barrier_semaphore()
    for step in range(1, n):
        pl.semaphore_signal(
            barrier, inc=1, device_id={"ctx": peers[step]}, device_id_type=pl.DeviceIdType.MESH
        )
    pl.semaphore_wait(barrier, n - 1)

    def remote(src, dst, send, recv, step):
        copy = pltpu.make_async_remote_copy(
            src_ref=src,
            dst_ref=dst,
            send_sem=send,
            recv_sem=recv,
            device_id={"ctx": peers[step]},
            device_id_type=pl.DeviceIdType.MESH,
        )
        copy.start()
        return copy

    sends, flags, gathers = {}, {}, {}
    for h in range(share):
        for index, (src, buf) in enumerate(tensors):
            for step in order:
                sends[index, h, step] = remote(
                    src.at[peers[step] * share + h],
                    buf.at[h, own_rows],
                    send_sem.at[index, h, step],
                    recv_sem.at[index, h, step],
                    step,
                )
            if h == 0 and index == 0:
                for step in order:
                    flags[step] = remote(
                        flag_out, flag_buf.at[me], flag_send.at[step], flag_recv.at[step], step
                    )

    w_copies = []
    for head in range(n * share):
        w_copies.append(
            pltpu.make_async_copy(
                w_hbm.at[head],
                w_buf.at[head % share, pl.ds((head // share) * width, width)],
                w_sem.at[head],
            )
        )
        w_copies[-1].start()
    state_copy = pltpu.make_async_copy(state_hbm, state_buf, state_sem)
    state_copy.start()

    def arrived(index, h):
        own[index, h].wait()
        for step in order:
            sends[index, h, step].wait_recv()

    def gather(h, block):
        if block is None:
            cut, slot = pl.ds(0, rows), 0
        else:
            cut, slot = pl.ds(block * TILE, TILE), block
        for step in order:
            gathers[h, slot, step] = remote(
                att_buf.at[h, cut, own_lanes],
                att_buf.at[h, cut, own_lanes],
                att_send.at[h, slot, step],
                att_recv.at[h, slot, step],
                step,
            )

    for h in range(share):
        arrived(0, h)
        arrived(1, h)
        if h == 0:
            for step in order:
                flags[step].wait_recv()
        for block in range(blocks):
            base = block * TILE
            chosen = q_buf[h, pl.ds(pl.multiple_of(me * rows, rows) + base, TILE), :].astype(jnp.float32) * flag[0:1, :]
            for step in order:
                start = pl.multiple_of(peers[step] * rows, rows) + base
                term = q_buf[h, pl.ds(start, TILE), :].astype(jnp.float32)
                chosen = chosen + term * flag_buf[peers[step], 0:1, :]
            scores = lax.dot_general(
                chosen.astype(jnp.bfloat16),
                k_buf[h],
                (((1,), (1,)), ((), ())),
                preferred_element_type=jnp.float32,
            )
            top = jnp.max(scores, axis=1, keepdims=True)
            weights = jnp.exp2((scores - top) * scale)
            total = jnp.sum(weights, axis=1, keepdims=True)
            probs[base : base + TILE, :] = weights.astype(jnp.bfloat16)
            inv_sum[base : base + TILE, :] = jnp.broadcast_to(1.0 / total, (TILE, width))
        arrived(2, h)
        last = h == share - 1
        for block in range(blocks):
            cut = slice(block * TILE, (block + 1) * TILE)
            weighted = jnp.dot(probs[cut, :], v_buf[h], preferred_element_type=jnp.float32)
            att_buf[h, cut, own_lanes] = (weighted * inv_sum[cut, :]).astype(jnp.bfloat16)
            if last:
                gather(h, block)
        if not last:
            gather(h, None)

    for copy in w_copies:
        copy.wait()
    state_copy.wait()

    for h in range(share - 1):
        for step in order:
            gathers[h, 0, step].wait_recv()

        def body(block, carry, h=h):
            cut = pl.ds(pl.multiple_of(block * TILE, TILE), TILE)
            product = jnp.dot(att_buf[h, cut, :], w_buf[h], preferred_element_type=jnp.float32)
            if h == 0:
                update[cut, :] = state_buf[cut, :].astype(jnp.float32) + product
            else:
                update[cut, :] = update[cut, :] + product
            return carry

        lax.fori_loop(0, blocks, body, 0)

    gain = gain_ref[...].astype(jnp.float32).reshape(1, -1)
    h = share - 1
    for block in range(blocks):
        for step in order:
            gathers[h, block, step].wait_recv()
        cut = slice(block * TILE, (block + 1) * TILE)
        mixed = jnp.dot(att_buf[h, cut, :], w_buf[h], preferred_element_type=jnp.float32)
        residual = update if share > 1 else state_buf
        mixed = residual[cut, :].astype(jnp.float32) + mixed
        mean = jnp.mean(mixed * mixed, axis=-1, keepdims=True)
        normed = mixed * lax.rsqrt(mean + 1e-06) * gain
        active = jnp.full(normed.shape, halt_ref[block * TILE] > STEP)
        kept = state_buf[cut, :].astype(jnp.float32)
        out_ref[cut, :] = jnp.where(active, normed, kept).astype(out_ref.dtype)

    for group in (sends, flags, gathers):
        for copy in group.values():
            copy.wait_send()


def split_heads(n, state_rows, q, k, v, halt_counts, out_weight, norm_gain):
    heads, rows, width = q.shape
    share = heads // n
    features = state_rows.shape[1]
    bf16, f32 = jnp.bfloat16, jnp.float32
    hbm = pl.BlockSpec(memory_space=pltpu.MemorySpace.HBM)
    vmem = pl.BlockSpec(memory_space=pltpu.VMEM)
    block = pltpu.VMEM((share, n * rows, width), bf16)
    dma = pltpu.SemaphoreType.DMA
    new_state = pl.pallas_call(
        functools.partial(split_kernel, n, share),
        out_shape=jax.ShapeDtypeStruct((rows, features), bf16),
        in_specs=[pl.BlockSpec(memory_space=pltpu.SMEM)] + [hbm] * 5 + [vmem],
        out_specs=vmem,
        scratch_shapes=[
            block,
            block,
            block,
            pltpu.VMEM((8, 128), f32),
            pltpu.VMEM((n, 8, 128), f32),
            pltpu.VMEM((rows, features), bf16),
            pltpu.VMEM((share, n * width, features), bf16),
            pltpu.VMEM((rows, n * rows), bf16),
            pltpu.VMEM((rows, width), f32),
            pltpu.VMEM((share, rows, n * width), bf16),
            pltpu.VMEM((rows, features), f32),
            dma((3, share, n)),
            dma((3, share, n)),
            dma((n,)),
            dma((n,)),
            dma((share, rows // TILE, n)),
            dma((share, rows // TILE, n)),
            dma((3, share)),
            dma((heads,)),
            dma,
        ],
        compiler_params=pltpu.CompilerParams(
            collective_id=0, has_side_effects=True, vmem_limit_bytes=60 * 1024 * 1024
        ),
    )(halt_counts, q, k, v, state_rows, out_weight, norm_gain)
    return new_state


def fold_heads(carry, queries, key_piece, value_piece, score_scale):
    running_max, running_sum, weighted = carry

    def per_head(head_items):
        query_head, key_head, value_head, max_head, sum_head, weighted_head = head_items
        scores = (
            lax.dot_general(
                query_head, key_head, (((1,), (1,)), ((), ())), preferred_element_type=jnp.float32
            )
            * score_scale
        )
        new_max = jnp.maximum(max_head, jnp.max(scores, axis=1))
        shrink = jnp.exp(max_head - new_max)
        exponents = jnp.exp(scores - new_max[:, None])
        sum_head = sum_head * shrink + jnp.sum(exponents, axis=1)
        weighted_head = weighted_head * shrink[:, None] + jnp.dot(
            exponents.astype(jnp.bfloat16), value_head, preferred_element_type=jnp.float32
        )
        return (new_max, sum_head, weighted_head)

    return lax.map(per_head, (queries, key_piece, value_piece, running_max, running_sum, weighted))


def empty_carry(head_count, query_count, head_width):
    return (
        jnp.full((head_count, query_count), -1e30, jnp.float32),
        jnp.zeros((head_count, query_count), jnp.float32),
        jnp.zeros((head_count, query_count, head_width), jnp.float32),
    )


def attend_keys(query_vectors, key_vectors, value_vectors, score_scale):
    head_count, row_count, head_width = query_vectors.shape
    initial = empty_carry(head_count, row_count, head_width)
    running_max, running_sum, weighted = fold_heads(
        initial,
        query_vectors,
        lax.all_gather(key_vectors, "ctx", axis=1, tiled=True),
        lax.all_gather(value_vectors, "ctx", axis=1, tiled=True),
        score_scale,
    )
    return (weighted / running_sum[..., None]).astype(jnp.bfloat16)


def on_device(
    state_rows, query_vectors, key_vectors, value_vectors, halt_counts, out_weight, norm_gain
):
    head_count, row_count, head_width = query_vectors.shape
    score_scale = head_width ** (-0.5)
    attended = attend_keys(query_vectors, key_vectors, value_vectors, score_scale)
    update = jnp.einsum("hqd,hde->qe", attended, out_weight, preferred_element_type=jnp.float32)
    mixed_sum = state_rows.astype(jnp.float32) + update
    normed = (
        mixed_sum
        * lax.rsqrt(jnp.mean(mixed_sum * mixed_sum, axis=-1, keepdims=True) + 1e-06)
        * norm_gain.astype(jnp.float32)
    )
    active = (halt_counts > STEP)[:, None]
    return jnp.where(active, normed.astype(jnp.bfloat16), state_rows)


def solution(mesh):
    n_ctx = mesh.shape["ctx"]

    def per_device(state_rows, q, k, v, halt_counts, out_weight, norm_gain):
        heads, rows, _ = q.shape
        one_owner = rows == (n_ctx - 1) * TILE
        if one_owner and heads % n_ctx == 0 and n_ctx & (n_ctx - 1) == 0:
            return split_heads(n_ctx, state_rows, q, k, v, halt_counts, out_weight, norm_gain)
        return on_device(state_rows, q, k, v, halt_counts, out_weight, norm_gain)

    placed = (
        P(("dp", "ctx"), None),
        P(None, ("dp", "ctx"), None),
        P(None, ("dp", "ctx"), None),
        P(None, ("dp", "ctx"), None),
        P(("dp", "ctx")),
        P(),
        P(),
    )
    return jax.shard_map(
        per_device, mesh=mesh, in_specs=placed, out_specs=P(("dp", "ctx"), None), check_vma=False
    )
```
